768 devices in a mesh: fsdp: 24 (over z, core), grp: 32 (over y, x).
Axes of the slice: x: 4, y: 8, z: 12, core: 2. Of those that a mesh axis runs over, the one named last changes fastest.
Arguments:
- grads: bfloat16 [384, 384, 2048], P('grp', 'fsdp')
- momentum: bfloat16 [384, 384, 2048], P('grp', 'fsdp'), may hold values from -6 to 6
- row_counts: int32 [384], P('grp'), may hold values from 128 to 384, as said below
Outputs:
- update: bfloat16 [384, 384, 2048], P('grp', 'fsdp')
- new_momentum: bfloat16 [384, 384, 2048], P('grp', 'fsdp')
The draws below stay inside these ranges and needn't reach their ends.
Inputs may be any that keep to these rules, and one draw needn't show every extreme that they name: `row_counts`: each entry is one, two or three times 384 // 3, and some entry equals 384.
All inputs are finite; a program needn't handle non-finite values.
Results may differ from the reference program's by a relative error of at most 0.007.
Values may be sent and summed in bfloat16 or wider, within the bound.
No kernel may reach another device: no remote copies, remote signals or barrier semaphores. Data moves between devices by JAX's collectives and lax.ppermute only.
A program may use at most 32 MiB of HBM per device.

```python
import math
import jax
import jax.numpy as jnp
from jax import lax

D = 2048
ROWS = 384
ITERS = 2
NMAT = 384


def draw_grads(key, part):
    first, second = jax.random.split(jax.random.fold_in(key, 11))
    matrix_ids = jnp.arange(NMAT, dtype=jnp.float32)[:, None, None]
    row_frac = jnp.arange(ROWS, dtype=jnp.float32)[None, :, None] / ROWS
    position = matrix_ids / NMAT
    rough = jax.random.uniform(first, (NMAT, ROWS, 1), minval=0.0, maxval=math.log(2.0))
    base = jax.random.normal(second, (NMAT, ROWS, D))
    scale = (1.0 + 4.0 * row_frac) * (1.0 + 0.5 * position) * jnp.exp(rough)
    return (base * scale).astype(jnp.bfloat16)


def draw_row_counts(key, part):
    level = jax.random.randint(jax.random.fold_in(key, 5), (NMAT,), 1, 5)
    level = jnp.minimum(level, 3)
    level = jnp.where(jnp.arange(NMAT) == 0, 3, level)
    return (level * (ROWS // 3)).astype(jnp.int32)


def block_levels(rng, extent, cuts, smallest, largest):
    level, own = 1.0, jax.random.fold_in(rng, 6)
    for dim, blocks in cuts:
        steps = jnp.exp(jax.random.uniform(jax.random.fold_in(own, dim), (blocks,), jnp.float32, smallest / len(cuts), largest / len(cuts)))
        level = level * jnp.repeat(steps, extent[dim] // blocks).reshape([-1 if axis == dim else 1 for axis in range(len(extent))])
    return level


def bell_draw(rng, dims, spread, limit, pieces=(), kind=jnp.bfloat16):
    drawn = spread * jax.random.normal(rng, dims, jnp.float32)
    if pieces:
        drawn = drawn * block_levels(rng, dims, pieces, -0.22, 0.18)
    return jnp.clip(drawn, -limit, limit).astype(kind)


def setup_inputs(seed: int = 0) -> dict:
    splits = jax.random.split(jax.random.key(seed), 4)
    return {
        "grads": draw_grads(jax.random.fold_in(splits[3], 71), 0),
        "momentum": bell_draw(splits[1], (NMAT, ROWS, D), 1.0, 6.0, ((0, 32), (1, 24))),
        "row_counts": draw_row_counts(jax.random.fold_in(splits[3], 71), 0),
    }


first_coef = 3.4445
second_coef = -4.775
third_coef = 2.0315

def orthogonal(matrix):
    frob = jnp.sqrt(jnp.sum(jnp.square(matrix.astype(jnp.float32))))
    current = (matrix.astype(jnp.float32) / (frob + 1e-07)).astype(jnp.bfloat16)
    for step in range(ITERS):
        gram = jnp.dot(current, current.T, preferred_element_type=jnp.float32).astype(jnp.bfloat16)
        square = jnp.dot(gram, gram, preferred_element_type=jnp.float32)
        poly = (second_coef * gram.astype(jnp.float32) + third_coef * square).astype(jnp.bfloat16)
        current = (first_coef * current.astype(jnp.float32) + jnp.dot(poly, current, preferred_element_type=jnp.float32)).astype(jnp.bfloat16)
    return current

def reference(grads, momentum, row_counts):
    row_ids = jnp.arange(ROWS, dtype=jnp.int32)
    live = row_ids[None, :, None] < row_counts[:, None, None]
    graded = jnp.where(live, grads.astype(jnp.float32), 0.0)
    total_rows = jnp.sum(row_counts).astype(jnp.float32)
    square_mean = jnp.sum(graded * graded) / (total_rows * D)
    clip = jnp.minimum(1.0, lax.rsqrt(square_mean + 1e-06))
    new_momentum = jnp.where(live, 0.95 * momentum.astype(jnp.float32) + clip * graded, 0.0).astype(jnp.bfloat16)
    result = lax.map(orthogonal, new_momentum)
    update = (0.2 * jnp.sqrt(jnp.float32(D)) * result.astype(jnp.float32)).astype(jnp.bfloat16)
    return (update, new_momentum)
```

```python
import jax
import jax.numpy as jnp
from jax import lax
from jax.sharding import Mesh
from jax.sharding import PartitionSpec as P

Z = "fsdp_0"
CORE = "fsdp_1"
FSDP = ("fsdp_0", "fsdp_1")
GRP = ("grp_0", "grp_1")
PLANE = ("fsdp_1", "grp_0", "grp_1")

first_coef = 3.4445
second_coef = -4.775
third_coef = 2.0315


def size_of(axes):
    size = 1
    for axis in axes:
        size *= lax.axis_size(axis)
    return size


def shared_sum(values, axes):
    lanes = lax.broadcasted_iota(jnp.int32, (1, 1, 128), 2)
    row = jnp.zeros((1, 1, 128), jnp.float32)
    for k, value in enumerate(values):
        row = jnp.where(lanes == k, value, row)
    count = size_of(axes)
    rows = lax.all_to_all(
        jnp.broadcast_to(row, (count, 1, 128)), axes, split_axis=0, concat_axis=0, tiled=True
    )
    return [jnp.sum(jnp.where(lanes == k, rows, 0.0)) for k in range(len(values))]


def product(left, right):
    return jnp.dot(left, right, preferred_element_type=jnp.float32)


def polynomials(gram):
    size = gram.shape[0]
    diagonal = lax.broadcasted_iota(jnp.int32, (size, size), 0) == lax.broadcasted_iota(
        jnp.int32, (size, size), 1
    )
    frob = jnp.sqrt(jnp.sum(jnp.where(diagonal, gram, 0.0)))
    inverse = 1.0 / (frob + 1e-07)
    gram0 = (gram * inverse * inverse).astype(jnp.bfloat16)
    poly0 = (
        second_coef * gram0.astype(jnp.float32) + third_coef * product(gram0, gram0)
    ).astype(jnp.bfloat16)
    half = first_coef * gram0.astype(jnp.float32) + product(poly0, gram0)
    gram1 = (first_coef * half + product(half.astype(jnp.bfloat16), poly0)).astype(jnp.bfloat16)
    poly1 = (
        second_coef * gram1.astype(jnp.float32) + third_coef * product(gram1, gram1)
    ).astype(jnp.bfloat16)
    return inverse, poly0, poly1


def applied(poly, x):
    return (first_coef * x.astype(jnp.float32) + product(poly, x)).astype(jnp.bfloat16)


def local(grads, momentum, row_counts):
    matrices, rows_here, width = grads.shape
    offset = lax.axis_index(FSDP) * rows_here
    row_ids = offset + lax.broadcasted_iota(jnp.int32, (1, rows_here, 1), 1)
    live = row_ids < row_counts[:, None, None]
    graded = jnp.where(live, grads.astype(jnp.float32), 0.0)
    (square_sum,) = shared_sum([jnp.sum(graded * graded)], (Z,))
    rows_in_group = jnp.sum(row_counts).astype(jnp.float32)
    square_sum, row_total = shared_sum([square_sum, rows_in_group], PLANE)
    row_total = row_total / lax.axis_size(CORE)
    clip = jnp.minimum(1.0, lax.rsqrt(square_sum / (row_total * width) + 1e-06))
    new_momentum = jnp.where(live, 0.95 * momentum.astype(jnp.float32) + clip * graded, 0.0).astype(
        jnp.bfloat16
    )
    cores = lax.axis_size(CORE)
    half_width = width // cores
    pieces = new_momentum.reshape(matrices, rows_here, cores, half_width).transpose(0, 2, 1, 3)
    pieces = pieces.reshape(matrices * cores, rows_here, half_width)
    owned = lax.all_to_all(pieces, FSDP, split_axis=0, concat_axis=0, tiled=True)
    owned = owned.reshape(-1, half_width)
    part = lax.dot_general(
        owned, owned, (((1,), (1,)), ((), ())), preferred_element_type=jnp.float32
    )
    gram = part + lax.ppermute(part, CORE, [(0, 1), (1, 0)])
    inverse, poly0, poly1 = polynomials(gram)
    x = (owned.astype(jnp.float32) * inverse).astype(jnp.bfloat16)
    x = applied(poly1, applied(poly0, x))
    x = (0.2 * jnp.sqrt(jnp.float32(width)) * x.astype(jnp.float32)).astype(jnp.bfloat16)
    back = lax.all_to_all(
        x.reshape(-1, rows_here, half_width), FSDP, split_axis=0, concat_axis=0, tiled=True
    )
    back = back.reshape(matrices, cores, rows_here, half_width).transpose(0, 2, 1, 3)
    update = back.reshape(matrices, rows_here, width)
    return (update, new_momentum)


def solution(mesh):
    torus = Mesh(mesh.devices.reshape(12, 2, 8, 4), ("fsdp_0", "fsdp_1", "grp_0", "grp_1"))
    in_specs = (P(GRP, FSDP, None), P(GRP, FSDP, None), P(GRP))
    out_specs = (P(GRP, FSDP, None), P(GRP, FSDP, None))
    return jax.shard_map(local, mesh=torus, in_specs=in_specs, out_specs=out_specs, check_vma=False)
```

```python
import jax
import jax.numpy as jnp
from jax import lax
from jax.experimental import pallas as pl
from jax.experimental.pallas import tpu as pltpu
from jax.sharding import Mesh
from jax.sharding import PartitionSpec as P

Z = "fsdp_0"
CORE = "fsdp_1"
FSDP = ("fsdp_0", "fsdp_1")
GRP = ("grp_0", "grp_1")
PLANE = ("fsdp_1", "grp_0", "grp_1")
LANES = 128
PARTS = 4
VMEM, SMEM, HBM = pltpu.VMEM, pltpu.SMEM, pltpu.HBM
KERNEL_VMEM = 16 * 1024 * 1024
FIRST_VMEM = 54500000

first_coef = 3.4445
second_coef = -4.775
third_coef = 2.0315


def size_of(axes):
    size = 1
    for axis in axes:
        size *= lax.axis_size(axis)
    return size


def exchanged(pieces, axes):
    return lax.all_to_all(pieces, axes, split_axis=0, concat_axis=0, tiled=True)


def on_core(body, out_shape, places, out_places, scratch=(), limit=KERNEL_VMEM):
    return pl.pallas_call(
        body,
        out_shape=out_shape,
        in_specs=[pl.BlockSpec(memory_space=place) for place in places],
        out_specs=[pl.BlockSpec(memory_space=place) for place in out_places],
        scratch_shapes=scratch,
        compiler_params=pltpu.CompilerParams(vmem_limit_bytes=limit),
    )


def product(left, right):
    return jnp.dot(left, right, preferred_element_type=jnp.float32)


def sum_kernel(
    offset_ref,
    counts_hbm,
    grads_hbm,
    momentum_hbm,
    out_ref,
    grads_ref,
    momentum_ref,
    counts_ref,
    sems,
    counts_sem,
    last_sem,
):
    matrices, rows_here, width = grads_ref.shape
    step = matrices // PARTS
    counted = pltpu.make_async_copy(counts_hbm, counts_ref, counts_sem)
    counted.start()
    copies = [
        pltpu.make_async_copy(
            grads_hbm.at[pl.ds(p * step, step)], grads_ref.at[pl.ds(p * step, step)], sems.at[p]
        )
        for p in range(PARTS)
    ]
    for copy in copies:
        copy.start()
    last = pltpu.make_async_copy(momentum_hbm, momentum_ref, last_sem)
    last.start()
    counted.wait()
    count = jnp.int32(0)
    total = jnp.zeros((rows_here, LANES), jnp.float32)
    for n in range(matrices):
        if n % step == 0:
            copies[n // step].wait()
        part = jnp.zeros((rows_here, LANES), jnp.float32)
        for k in range(width // LANES):
            graded = grads_ref[n, :, k * LANES : (k + 1) * LANES].astype(jnp.float32)
            part = part + graded * graded
        total = total + jnp.where(counts_ref[n] > offset_ref[0], part, 0.0)
        count = count + counts_ref[n]
    row = jnp.sum(total, axis=0, keepdims=True)[None]
    out_ref[:, 0:1, :] = jnp.broadcast_to(row, (out_ref.shape[0], 1, LANES))
    out_ref[:, 1:2, :] = jnp.full((out_ref.shape[0], 1, LANES), count.astype(jnp.float32))
    last.wait()
    for n in range(matrices):

        @pl.when(counts_ref[n] <= offset_ref[0])
        def _():
            grads_ref[n] = jnp.zeros((rows_here, width), jnp.bfloat16)
            momentum_ref[n] = jnp.zeros((rows_here, width), jnp.bfloat16)


def pass_on_kernel(sums_ref, out_ref):
    row = jnp.sum(sums_ref[:, 0:1, :], axis=0, keepdims=True)
    out_ref[:, 0:1, :] = jnp.broadcast_to(row, (out_ref.shape[0], 1, LANES))
    out_ref[:, 1:2, :] = jnp.broadcast_to(sums_ref[0:1, 1:2, :], (out_ref.shape[0], 1, LANES))


def momentum_kernel(cores, sums_ref, grads_ref, momentum_ref, out_ref):
    matrices, _, width = grads_ref.shape
    square_sum = jnp.sum(jnp.sum(sums_ref[:, 0:1, :], axis=0), axis=1, keepdims=True)
    row_total = jnp.sum(sums_ref[:, 1:2, :], axis=0)[:, 0:1] * (1.0 / cores)
    clip = jnp.minimum(1.0, 1.0 / jnp.sqrt(square_sum / (row_total * width) + 1e-06))
    for n in range(matrices):
        mixed = 0.95 * momentum_ref[n].astype(jnp.float32) + clip * grads_ref[n].astype(jnp.float32)
        out_ref[n] = mixed.astype(jnp.bfloat16)


def orthogonal_kernel(scale, mine_ref, other_ref, momentum_ref, out_ref, momentum_hbm, x_ref, sem):
    written = pltpu.make_async_copy(momentum_ref, momentum_hbm, sem)
    written.start()
    here = mine_ref.shape[0]
    size = 2 * here
    x_ref[:here] = mine_ref[...]
    x_ref[here:] = other_ref[...]
    gram = lax.dot_general(
        x_ref[...], x_ref[...], (((1,), (1,)), ((), ())), preferred_element_type=jnp.float32
    )
    diagonal = lax.broadcasted_iota(jnp.int32, (size, size), 0) == lax.broadcasted_iota(
        jnp.int32, (size, size), 1
    )
    frob = jnp.sqrt(
        jnp.sum(
            jnp.sum(jnp.where(diagonal, gram, 0.0), axis=0, keepdims=True), axis=1, keepdims=True
        )
    )
    inverse = 1.0 / (frob + 1e-07)
    gram0 = ((gram * inverse) * inverse).astype(jnp.bfloat16)
    poly0 = (
        second_coef * gram0.astype(jnp.float32) + third_coef * product(gram0, gram0)
    ).astype(jnp.bfloat16)
    half = first_coef * gram0.astype(jnp.float32) + product(poly0, gram0)
    gram1 = (first_coef * half + product(half.astype(jnp.bfloat16), poly0)).astype(jnp.bfloat16)
    poly1 = (
        second_coef * gram1[:here].astype(jnp.float32) + third_coef * product(gram1[:here], gram1)
    ).astype(jnp.bfloat16)
    x_ref[...] = (x_ref[...].astype(jnp.float32) * inverse).astype(jnp.bfloat16)
    x_ref[...] = (
        first_coef * x_ref[...].astype(jnp.float32) + product(poly0, x_ref[...])
    ).astype(jnp.bfloat16)
    x = (
        first_coef * x_ref[:here].astype(jnp.float32) + product(poly1, x_ref[...])
    ).astype(jnp.bfloat16)
    out_ref[...] = (scale * x.astype(jnp.float32)).astype(jnp.bfloat16)
    written.wait()


def local(grads, momentum, row_counts):
    matrices, rows_here, width = grads.shape
    cores = lax.axis_size(CORE)
    offset = (lax.axis_index(FSDP) * rows_here).astype(jnp.int32).reshape(1)
    stack = jax.ShapeDtypeStruct(grads.shape, jnp.bfloat16)
    sums, grads, momentum = on_core(
        sum_kernel,
        [jax.ShapeDtypeStruct((lax.axis_size(Z), 2, LANES), jnp.float32), stack, stack],
        [SMEM, HBM, HBM, HBM],
        [VMEM, VMEM, VMEM],
        [
            pltpu.SMEM((matrices,), jnp.int32),
            pltpu.SemaphoreType.DMA((PARTS,)),
            pltpu.SemaphoreType.DMA,
            pltpu.SemaphoreType.DMA,
        ],
        FIRST_VMEM,
    )(offset, row_counts, grads, momentum)
    sums = exchanged(sums, (Z,))
    (sums,) = on_core(
        pass_on_kernel,
        [jax.ShapeDtypeStruct((size_of(PLANE), 2, LANES), jnp.float32)],
        [VMEM],
        [VMEM],
    )(sums)
    sums = exchanged(sums, PLANE)
    (new_momentum,) = on_core(
        lambda *refs: momentum_kernel(cores, *refs), [stack], [VMEM, VMEM, VMEM], [VMEM]
    )(sums, grads, momentum)
    mine = exchanged(new_momentum, (Z,)).reshape(-1, width)
    other = lax.ppermute(mine, CORE, [(0, 1), (1, 0)])
    scale = 0.2 * width**0.5
    result, new_momentum = on_core(
        lambda *refs: orthogonal_kernel(scale, *refs),
        [jax.ShapeDtypeStruct(mine.shape, jnp.bfloat16), stack],
        [VMEM, VMEM, VMEM],
        [VMEM, HBM],
        [pltpu.VMEM((2 * mine.shape[0], width), jnp.bfloat16), pltpu.SemaphoreType.DMA],
    )(mine, other, new_momentum)
    update = exchanged(result.reshape(grads.shape), (Z,))
    return (update, new_momentum)


def solution(mesh):
    torus = Mesh(mesh.devices.reshape(12, 2, 8, 4), ("fsdp_0", "fsdp_1", "grp_0", "grp_1"))
    in_specs = (P(GRP, FSDP, None), P(GRP, FSDP, None), P(GRP))
    out_specs = (P(GRP, FSDP, None), P(GRP, FSDP, None))
    return jax.shard_map(local, mesh=torus, in_specs=in_specs, out_specs=out_specs, check_vma=False)
```

```python
import jax
import jax.numpy as jnp
from jax import lax
from jax.experimental import pallas as pl
from jax.experimental.pallas import tpu as pltpu
from jax.sharding import Mesh
from jax.sharding import PartitionSpec as P

Z = "fsdp_0"
CORE = "fsdp_1"
FSDP = ("fsdp_0", "fsdp_1")
GRP = ("grp_0", "grp_1")
FIRST = ("fsdp_1", "grp_0", "grp_1")
SECOND = ("fsdp_0",)
LANES = 128
PARTS = 4
VMEM, SMEM, HBM = pltpu.VMEM, pltpu.SMEM, pltpu.HBM
KERNEL_VMEM = 16 * 1024 * 1024
FIRST_VMEM = 54500000

first_coef = 3.4445
second_coef = -4.775
third_coef = 2.0315


def size_of(axes):
    size = 1
    for axis in axes:
        size *= lax.axis_size(axis)
    return size


def exchanged(pieces, axes):
    return lax.all_to_all(pieces, axes, split_axis=0, concat_axis=0, tiled=True)


def on_core(body, out_shape, places, out_places, scratch=(), limit=KERNEL_VMEM):
    return pl.pallas_call(
        body,
        out_shape=out_shape,
        in_specs=[pl.BlockSpec(memory_space=place) for place in places],
        out_specs=[pl.BlockSpec(memory_space=place) for place in out_places],
        scratch_shapes=scratch,
        compiler_params=pltpu.CompilerParams(vmem_limit_bytes=limit),
    )


def product(left, right):
    return jnp.dot(left, right, preferred_element_type=jnp.float32)


def sum_kernel(
    offset_ref,
    counts_hbm,
    grads_hbm,
    momentum_hbm,
    out_ref,
    grads_ref,
    momentum_ref,
    counts_ref,
    sems,
    counts_sem,
    last_sem,
):
    matrices, rows_here, width = grads_ref.shape
    step = matrices // PARTS
    counted = pltpu.make_async_copy(counts_hbm, counts_ref, counts_sem)
    counted.start()
    copies = [
        pltpu.make_async_copy(
            grads_hbm.at[pl.ds(p * step, step)], grads_ref.at[pl.ds(p * step, step)], sems.at[p]
        )
        for p in range(PARTS)
    ]
    for copy in copies:
        copy.start()
    last = pltpu.make_async_copy(momentum_hbm, momentum_ref, last_sem)
    last.start()
    counted.wait()
    count = jnp.int32(0)
    total = jnp.zeros((rows_here, LANES), jnp.float32)
    for n in range(matrices):
        if n % step == 0:
            copies[n // step].wait()
        part = jnp.zeros((rows_here, LANES), jnp.float32)
        for k in range(width // LANES):
            graded = grads_ref[n, :, k * LANES : (k + 1) * LANES].astype(jnp.float32)
            part = part + graded * graded
        total = total + jnp.where(counts_ref[n] > offset_ref[0], part, 0.0)
        count = count + counts_ref[n]
    row = jnp.sum(total, axis=0, keepdims=True)[None]
    out_ref[:, 0:1, :] = jnp.broadcast_to(row, (out_ref.shape[0], 1, LANES))
    out_ref[:, 1:2, :] = jnp.full((out_ref.shape[0], 1, LANES), count.astype(jnp.float32))
    last.wait()
    for n in range(matrices):

        @pl.when(counts_ref[n] <= offset_ref[0])
        def _():
            grads_ref[n] = jnp.zeros((rows_here, width), jnp.bfloat16)
            momentum_ref[n] = jnp.zeros((rows_here, width), jnp.bfloat16)


def pass_on_kernel(sums_ref, out_ref):
    out_ref[...] = jnp.broadcast_to(jnp.sum(sums_ref[...], axis=0, keepdims=True), out_ref.shape)


def momentum_kernel(tellers, sums_ref, grads_ref, momentum_ref, out_ref):
    matrices, _, width = grads_ref.shape
    square_sum = jnp.sum(jnp.sum(sums_ref[:, 0:1, :], axis=0), axis=1, keepdims=True)
    row_total = jnp.sum(sums_ref[:, 1:2, :], axis=0)[:, 0:1] / tellers
    clip = jnp.minimum(1.0, 1.0 / jnp.sqrt(square_sum / (row_total * width) + 1e-06))
    for n in range(matrices):
        mixed = 0.95 * momentum_ref[n].astype(jnp.float32) + clip * grads_ref[n].astype(jnp.float32)
        out_ref[n] = mixed.astype(jnp.bfloat16)


def orthogonal_kernel(scale, mine_ref, other_ref, momentum_ref, out_ref, momentum_hbm, x_ref, sem):
    written = pltpu.make_async_copy(momentum_ref, momentum_hbm, sem)
    written.start()
    here = mine_ref.shape[0]
    size = 2 * here
    x_ref[:here] = mine_ref[...]
    x_ref[here:] = other_ref[...]
    gram = lax.dot_general(
        x_ref[...], x_ref[...], (((1,), (1,)), ((), ())), preferred_element_type=jnp.float32
    )
    diagonal = lax.broadcasted_iota(jnp.int32, (size, size), 0) == lax.broadcasted_iota(
        jnp.int32, (size, size), 1
    )
    frob = jnp.sqrt(
        jnp.sum(
            jnp.sum(jnp.where(diagonal, gram, 0.0), axis=0, keepdims=True), axis=1, keepdims=True
        )
    )
    inverse = 1.0 / (frob + 1e-07)
    gram0 = ((gram * inverse) * inverse).astype(jnp.bfloat16)
    poly0 = (
        second_coef * gram0.astype(jnp.float32) + third_coef * product(gram0, gram0)
    ).astype(jnp.bfloat16)
    half = first_coef * gram0.astype(jnp.float32) + product(poly0, gram0)
    gram1 = (first_coef * half + product(half.astype(jnp.bfloat16), poly0)).astype(jnp.bfloat16)
    poly1 = (
        second_coef * gram1[:here].astype(jnp.float32) + third_coef * product(gram1[:here], gram1)
    ).astype(jnp.bfloat16)
    x_ref[...] = (x_ref[...].astype(jnp.float32) * inverse).astype(jnp.bfloat16)
    x_ref[...] = (
        first_coef * x_ref[...].astype(jnp.float32) + product(poly0, x_ref[...])
    ).astype(jnp.bfloat16)
    x = (
        first_coef * x_ref[:here].astype(jnp.float32) + product(poly1, x_ref[...])
    ).astype(jnp.bfloat16)
    out_ref[...] = (scale * x.astype(jnp.float32)).astype(jnp.bfloat16)
    written.wait()


def local(grads, momentum, row_counts):
    matrices, rows_here, width = grads.shape
    tellers = size_of(FSDP)
    offset = (lax.axis_index(FSDP) * rows_here).astype(jnp.int32).reshape(1)
    stack = jax.ShapeDtypeStruct(grads.shape, jnp.bfloat16)
    sums, grads, momentum = on_core(
        sum_kernel,
        [jax.ShapeDtypeStruct((size_of(FIRST), 2, LANES), jnp.float32), stack, stack],
        [SMEM, HBM, HBM, HBM],
        [VMEM, VMEM, VMEM],
        [
            pltpu.SMEM((matrices,), jnp.int32),
            pltpu.SemaphoreType.DMA((PARTS,)),
            pltpu.SemaphoreType.DMA,
            pltpu.SemaphoreType.DMA,
        ],
        FIRST_VMEM,
    )(offset, row_counts, grads, momentum)
    sums = exchanged(sums, FIRST)
    (sums,) = on_core(
        pass_on_kernel,
        [jax.ShapeDtypeStruct((size_of(SECOND), 2, LANES), jnp.float32)],
        [VMEM],
        [VMEM],
    )(sums)
    sums = exchanged(sums, SECOND)
    (new_momentum,) = on_core(
        lambda *refs: momentum_kernel(tellers, *refs), [stack], [VMEM, VMEM, VMEM], [VMEM]
    )(sums, grads, momentum)
    mine = exchanged(new_momentum, (Z,)).reshape(-1, width)
    other = lax.ppermute(mine, CORE, [(0, 1), (1, 0)])
    scale = 0.2 * width**0.5
    result, new_momentum = on_core(
        lambda *refs: orthogonal_kernel(scale, *refs),
        [jax.ShapeDtypeStruct(mine.shape, jnp.bfloat16), stack],
        [VMEM, VMEM, VMEM],
        [VMEM, HBM],
        [pltpu.VMEM((2 * mine.shape[0], width), jnp.bfloat16), pltpu.SemaphoreType.DMA],
    )(mine, other, new_momentum)
    update = exchanged(result.reshape(grads.shape), (Z,))
    return (update, new_momentum)


def solution(mesh):
    torus = Mesh(mesh.devices.reshape(12, 2, 8, 4), ("fsdp_0", "fsdp_1", "grp_0", "grp_1"))
    in_specs = (P(GRP, FSDP, None), P(GRP, FSDP, None), P(GRP))
    out_specs = (P(GRP, FSDP, None), P(GRP, FSDP, None))
    return jax.shard_map(local, mesh=torus, in_specs=in_specs, out_specs=out_specs, check_vma=False)
```

```python
import jax
import jax.numpy as jnp
from jax import lax
from jax.experimental import pallas as pl
from jax.experimental.pallas import tpu as pltpu
from jax.sharding import Mesh
from jax.sharding import PartitionSpec as P

Z = "fsdp_0"
CORE = "fsdp_1"
FSDP = ("fsdp_0", "fsdp_1")
GRP = ("grp_0", "grp_1")
FIRST = ("fsdp_1", "grp_0", "grp_1")
SECOND = ("fsdp_0",)
LANES = 128
PARTS = 4
VMEM, SMEM, HBM = pltpu.VMEM, pltpu.SMEM, pltpu.HBM
KERNEL_VMEM = 16 * 1024 * 1024
FIRST_VMEM = 54500000

first_coef = 3.4445
second_coef = -4.775
third_coef = 2.0315


def size_of(axes):
    size = 1
    for axis in axes:
        size *= lax.axis_size(axis)
    return size


def exchanged(pieces, axes):
    return lax.all_to_all(pieces, axes, split_axis=0, concat_axis=0, tiled=True)


def on_core(body, out_shape, places, out_places, scratch=(), limit=KERNEL_VMEM):
    return pl.pallas_call(
        body,
        out_shape=out_shape,
        in_specs=[pl.BlockSpec(memory_space=place) for place in places],
        out_specs=[pl.BlockSpec(memory_space=place) for place in out_places],
        scratch_shapes=scratch,
        compiler_params=pltpu.CompilerParams(vmem_limit_bytes=limit),
    )


def product(left, right):
    return jnp.dot(left, right, preferred_element_type=jnp.float32)


def sum_kernel(
    offset_ref,
    counts_hbm,
    grads_hbm,
    momentum_hbm,
    out_ref,
    grads_ref,
    momentum_ref,
    counts_ref,
    sems,
    counts_sem,
    last_sem,
):
    matrices, rows_here, width = grads_ref.shape
    step = matrices // PARTS
    counted = pltpu.make_async_copy(counts_hbm, counts_ref, counts_sem)
    counted.start()
    copies = [
        pltpu.make_async_copy(
            grads_hbm.at[pl.ds(p * step, step)], grads_ref.at[pl.ds(p * step, step)], sems.at[p]
        )
        for p in range(PARTS)
    ]
    for copy in copies:
        copy.start()
    last = pltpu.make_async_copy(momentum_hbm, momentum_ref, last_sem)
    last.start()
    counted.wait()
    count = jnp.int32(0)
    total = jnp.zeros((rows_here, LANES), jnp.float32)
    for n in range(matrices):
        if n % step == 0:
            copies[n // step].wait()
        part = jnp.zeros((rows_here, LANES), jnp.float32)
        for k in range(width // LANES):
            graded = grads_ref[n, :, k * LANES : (k + 1) * LANES].astype(jnp.float32)
            part = part + graded * graded
        total = total + jnp.where(counts_ref[n] > offset_ref[0], part, 0.0)
        count = count + counts_ref[n]
    row = jnp.sum(total, axis=0, keepdims=True)[None]
    out_ref[:, 0:1, :] = jnp.broadcast_to(row, (out_ref.shape[0], 1, LANES))
    out_ref[:, 1:2, :] = jnp.full((out_ref.shape[0], 1, LANES), count.astype(jnp.float32))
    last.wait()
    for n in range(matrices):

        @pl.when(counts_ref[n] <= offset_ref[0])
        def _():
            grads_ref[n] = jnp.zeros((rows_here, width), jnp.bfloat16)
            momentum_ref[n] = jnp.zeros((rows_here, width), jnp.bfloat16)


def pass_on_kernel(sums_ref, out_ref):
    out_ref[...] = jnp.broadcast_to(jnp.sum(sums_ref[...], axis=0, keepdims=True), out_ref.shape)


def momentum_kernel(tellers, sums_ref, grads_ref, momentum_ref, out_ref):
    matrices, _, width = grads_ref.shape
    square_sum = jnp.sum(jnp.sum(sums_ref[:, 0:1, :], axis=0), axis=1, keepdims=True)
    row_total = jnp.sum(sums_ref[:, 1:2, :], axis=0)[:, 0:1] / tellers
    clip = jnp.minimum(1.0, 1.0 / jnp.sqrt(square_sum / (row_total * width) + 1e-06))
    for n in range(matrices):
        mixed = 0.95 * momentum_ref[n].astype(jnp.float32) + clip * grads_ref[n].astype(jnp.float32)
        out_ref[n] = mixed.astype(jnp.bfloat16)


def product_by_rows(left, right):
    return lax.dot_general(
        left, right, (((1,), (1,)), ((), ())), preferred_element_type=jnp.float32
    )


def own_gram_kernel(mine_ref, gram_ref):
    gram_ref[...] = product_by_rows(mine_ref[...], mine_ref[...])


def orthogonal_kernel(
    scale,
    mine_ref,
    other_ref,
    own_ref,
    momentum_ref,
    out_ref,
    momentum_hbm,
    x_ref,
    gram_ref,
    sem,
):
    written = pltpu.make_async_copy(momentum_ref, momentum_hbm, sem)
    written.start()
    here = mine_ref.shape[0]
    size = 2 * here
    x_ref[:here] = mine_ref[...]
    x_ref[here:] = other_ref[...]
    rest = product_by_rows(other_ref[...], x_ref[...])
    gram_ref[:here, :here] = own_ref[...]
    gram_ref[here:] = rest
    gram_ref[:here, here:] = rest[:, :here].T
    gram = gram_ref[...]
    diagonal = lax.broadcasted_iota(jnp.int32, (size, size), 0) == lax.broadcasted_iota(
        jnp.int32, (size, size), 1
    )
    frob = jnp.sqrt(
        jnp.sum(
            jnp.sum(jnp.where(diagonal, gram, 0.0), axis=0, keepdims=True), axis=1, keepdims=True
        )
    )
    inverse = 1.0 / (frob + 1e-07)
    gram0 = ((gram * inverse) * inverse).astype(jnp.bfloat16)
    poly0 = (
        second_coef * gram0.astype(jnp.float32) + third_coef * product(gram0, gram0)
    ).astype(jnp.bfloat16)
    half = first_coef * gram0.astype(jnp.float32) + product(poly0, gram0)
    gram1 = (first_coef * half + product(half.astype(jnp.bfloat16), poly0)).astype(jnp.bfloat16)
    poly1 = (
        second_coef * gram1[:here].astype(jnp.float32) + third_coef * product(gram1[:here], gram1)
    ).astype(jnp.bfloat16)
    x_ref[...] = (x_ref[...].astype(jnp.float32) * inverse).astype(jnp.bfloat16)
    x_ref[...] = (
        first_coef * x_ref[...].astype(jnp.float32) + product(poly0, x_ref[...])
    ).astype(jnp.bfloat16)
    x = (
        first_coef * x_ref[:here].astype(jnp.float32) + product(poly1, x_ref[...])
    ).astype(jnp.bfloat16)
    out_ref[...] = (scale * x.astype(jnp.float32)).astype(jnp.bfloat16)
    written.wait()


def local(grads, momentum, row_counts):
    matrices, rows_here, width = grads.shape
    tellers = size_of(FSDP)
    offset = (lax.axis_index(FSDP) * rows_here).astype(jnp.int32).reshape(1)
    stack = jax.ShapeDtypeStruct(grads.shape, jnp.bfloat16)
    sums, grads, momentum = on_core(
        sum_kernel,
        [jax.ShapeDtypeStruct((size_of(FIRST), 2, LANES), jnp.float32), stack, stack],
        [SMEM, HBM, HBM, HBM],
        [VMEM, VMEM, VMEM],
        [
            pltpu.SMEM((matrices,), jnp.int32),
            pltpu.SemaphoreType.DMA((PARTS,)),
            pltpu.SemaphoreType.DMA,
            pltpu.SemaphoreType.DMA,
        ],
        FIRST_VMEM,
    )(offset, row_counts, grads, momentum)
    sums = exchanged(sums, FIRST)
    (sums,) = on_core(
        pass_on_kernel,
        [jax.ShapeDtypeStruct((size_of(SECOND), 2, LANES), jnp.float32)],
        [VMEM],
        [VMEM],
    )(sums)
    sums = exchanged(sums, SECOND)
    (new_momentum,) = on_core(
        lambda *refs: momentum_kernel(tellers, *refs), [stack], [VMEM, VMEM, VMEM], [VMEM]
    )(sums, grads, momentum)
    mine = exchanged(new_momentum, (Z,)).reshape(-1, width)
    other = lax.ppermute(mine, CORE, [(0, 1), (1, 0)])
    here = mine.shape[0]
    (own,) = on_core(
        own_gram_kernel, [jax.ShapeDtypeStruct((here, here), jnp.float32)], [VMEM], [VMEM]
    )(mine)
    scale = 0.2 * width**0.5
    result, new_momentum = on_core(
        lambda *refs: orthogonal_kernel(scale, *refs),
        [jax.ShapeDtypeStruct(mine.shape, jnp.bfloat16), stack],
        [VMEM, VMEM, VMEM, VMEM],
        [VMEM, HBM],
        [
            pltpu.VMEM((2 * here, width), jnp.bfloat16),
            pltpu.VMEM((2 * here, 2 * here), jnp.float32),
            pltpu.SemaphoreType.DMA,
        ],
    )(mine, other, own, new_momentum)
    update = exchanged(result.reshape(grads.shape), (Z,))
    return (update, new_momentum)


def solution(mesh):
    torus = Mesh(mesh.devices.reshape(12, 2, 8, 4), ("fsdp_0", "fsdp_1", "grp_0", "grp_1"))
    in_specs = (P(GRP, FSDP, None), P(GRP, FSDP, None), P(GRP))
    out_specs = (P(GRP, FSDP, None), P(GRP, FSDP, None))
    return jax.shard_map(local, mesh=torus, in_specs=in_specs, out_specs=out_specs, check_vma=False)
```

```python
import jax
import jax.numpy as jnp
from jax import lax
from jax.experimental import pallas as pl
from jax.experimental.pallas import tpu as pltpu
from jax.sharding import Mesh
from jax.sharding import PartitionSpec as P

Z = "fsdp_0"
CORE = "fsdp_1"
FSDP = ("fsdp_0", "fsdp_1")
GRP = ("grp_0", "grp_1")
FIRST = ("fsdp_1", "grp_0", "grp_1")
SECOND = ("fsdp_0",)
LANES = 128
PARTS = 4
VMEM, SMEM, HBM = pltpu.VMEM, pltpu.SMEM, pltpu.HBM
KERNEL_VMEM = 16 * 1024 * 1024
FIRST_VMEM = 54500000

first_coef = 3.4445
second_coef = -4.775
third_coef = 2.0315


def size_of(axes):
    size = 1
    for axis in axes:
        size *= lax.axis_size(axis)
    return size


def exchanged(pieces, axes):
    return lax.all_to_all(pieces, axes, split_axis=0, concat_axis=0, tiled=True)


def on_core(body, out_shape, places, out_places, scratch=(), limit=KERNEL_VMEM):
    return pl.pallas_call(
        body,
        out_shape=out_shape,
        in_specs=[pl.BlockSpec(memory_space=place) for place in places],
        out_specs=[pl.BlockSpec(memory_space=place) for place in out_places],
        scratch_shapes=scratch,
        compiler_params=pltpu.CompilerParams(vmem_limit_bytes=limit),
    )


def product(left, right):
    return jnp.dot(left, right, preferred_element_type=jnp.float32)


def sum_kernel(
    offset_ref,
    counts_hbm,
    grads_hbm,
    momentum_hbm,
    out_ref,
    grads_ref,
    momentum_ref,
    counts_ref,
    sems,
    counts_sem,
    last_sem,
):
    matrices, rows_here, width = grads_ref.shape
    step = matrices // PARTS
    counted = pltpu.make_async_copy(counts_hbm, counts_ref, counts_sem)
    counted.start()
    copies = [
        pltpu.make_async_copy(
            grads_hbm.at[pl.ds(p * step, step)], grads_ref.at[pl.ds(p * step, step)], sems.at[p]
        )
        for p in range(PARTS)
    ]
    for copy in copies:
        copy.start()
    last = pltpu.make_async_copy(momentum_hbm, momentum_ref, last_sem)
    last.start()
    counted.wait()
    count = jnp.int32(0)
    total = jnp.zeros((rows_here, LANES), jnp.float32)
    for n in range(matrices):
        if n % step == 0:
            copies[n // step].wait()
        part = jnp.zeros((rows_here, LANES), jnp.float32)
        for k in range(width // LANES):
            graded = grads_ref[n, :, k * LANES : (k + 1) * LANES].astype(jnp.float32)
            part = part + graded * graded
        total = total + jnp.where(counts_ref[n] > offset_ref[0], part, 0.0)
        count = count + counts_ref[n]
    row = jnp.sum(total, axis=0, keepdims=True)[None]
    out_ref[:, 0:1, :] = jnp.broadcast_to(row, (out_ref.shape[0], 1, LANES))
    out_ref[:, 1:2, :] = jnp.full((out_ref.shape[0], 1, LANES), count.astype(jnp.float32))
    last.wait()
    for n in range(matrices):

        @pl.when(counts_ref[n] <= offset_ref[0])
        def _():
            grads_ref[n] = jnp.zeros((rows_here, width), jnp.bfloat16)
            momentum_ref[n] = jnp.zeros((rows_here, width), jnp.bfloat16)


def pass_on_kernel(sums_ref, out_ref):
    out_ref[...] = jnp.broadcast_to(jnp.sum(sums_ref[...], axis=0, keepdims=True), out_ref.shape)


def momentum_kernel(tellers, sums_ref, grads_ref, momentum_ref, out_ref):
    matrices, _, width = grads_ref.shape
    square_sum = jnp.sum(jnp.sum(sums_ref[:, 0:1, :], axis=0), axis=1, keepdims=True)
    row_total = jnp.sum(sums_ref[:, 1:2, :], axis=0)[:, 0:1] / tellers
    clip = jnp.minimum(1.0, 1.0 / jnp.sqrt(square_sum / (row_total * width) + 1e-06))
    for n in range(matrices):
        mixed = 0.95 * momentum_ref[n].astype(jnp.float32) + clip * grads_ref[n].astype(jnp.float32)
        out_ref[n] = mixed.astype(jnp.bfloat16)


def product_by_rows(left, right):
    return lax.dot_general(
        left, right, (((1,), (1,)), ((), ())), preferred_element_type=jnp.float32
    )


def own_gram_kernel(mine_ref, gram_ref):
    gram_ref[...] = product_by_rows(mine_ref[...], mine_ref[...])


def orthogonal_kernel(
    scale,
    mine_ref,
    other_ref,
    own_ref,
    momentum_ref,
    out_ref,
    momentum_hbm,
    x_ref,
    gram_ref,
    sem,
):
    written = pltpu.make_async_copy(momentum_ref, momentum_hbm, sem)
    written.start()
    here = mine_ref.shape[0]
    size = 2 * here
    mixed = product_by_rows(other_ref[...], mine_ref[...])
    gram_ref[:here, :here] = own_ref[...]
    gram_ref[here:, :here] = mixed
    gram_ref[:here, here:] = mixed.T
    gram_ref[here:, here:] = product_by_rows(other_ref[...], other_ref[...])
    gram = gram_ref[...]
    diagonal = lax.broadcasted_iota(jnp.int32, (size, size), 0) == lax.broadcasted_iota(
        jnp.int32, (size, size), 1
    )
    frob = jnp.sqrt(
        jnp.sum(
            jnp.sum(jnp.where(diagonal, gram, 0.0), axis=0, keepdims=True), axis=1, keepdims=True
        )
    )
    inverse = 1.0 / (frob + 1e-07)
    gram0 = ((gram * inverse) * inverse).astype(jnp.bfloat16)
    poly0 = (
        second_coef * gram0.astype(jnp.float32) + third_coef * product(gram0, gram0)
    ).astype(jnp.bfloat16)
    half = first_coef * gram0.astype(jnp.float32) + product(poly0, gram0)
    gram1 = (first_coef * half + product(half.astype(jnp.bfloat16), poly0)).astype(jnp.bfloat16)
    poly1 = (
        second_coef * gram1[:here].astype(jnp.float32) + third_coef * product(gram1[:here], gram1)
    ).astype(jnp.bfloat16)
    x_ref[:here] = (mine_ref[...].astype(jnp.float32) * inverse).astype(jnp.bfloat16)
    x_ref[here:] = (other_ref[...].astype(jnp.float32) * inverse).astype(jnp.bfloat16)
    x_ref[...] = (
        first_coef * x_ref[...].astype(jnp.float32) + product(poly0, x_ref[...])
    ).astype(jnp.bfloat16)
    x = (
        first_coef * x_ref[:here].astype(jnp.float32) + product(poly1, x_ref[...])
    ).astype(jnp.bfloat16)
    out_ref[...] = (scale * x.astype(jnp.float32)).astype(jnp.bfloat16)
    written.wait()


def local(grads, momentum, row_counts):
    matrices, rows_here, width = grads.shape
    tellers = size_of(FSDP)
    offset = (lax.axis_index(FSDP) * rows_here).astype(jnp.int32).reshape(1)
    stack = jax.ShapeDtypeStruct(grads.shape, jnp.bfloat16)
    sums, grads, momentum = on_core(
        sum_kernel,
        [jax.ShapeDtypeStruct((size_of(FIRST), 2, LANES), jnp.float32), stack, stack],
        [SMEM, HBM, HBM, HBM],
        [VMEM, VMEM, VMEM],
        [
            pltpu.SMEM((matrices,), jnp.int32),
            pltpu.SemaphoreType.DMA((PARTS,)),
            pltpu.SemaphoreType.DMA,
            pltpu.SemaphoreType.DMA,
        ],
        FIRST_VMEM,
    )(offset, row_counts, grads, momentum)
    sums = exchanged(sums, FIRST)
    (sums,) = on_core(
        pass_on_kernel,
        [jax.ShapeDtypeStruct((size_of(SECOND), 2, LANES), jnp.float32)],
        [VMEM],
        [VMEM],
    )(sums)
    sums = exchanged(sums, SECOND)
    (new_momentum,) = on_core(
        lambda *refs: momentum_kernel(tellers, *refs), [stack], [VMEM, VMEM, VMEM], [VMEM]
    )(sums, grads, momentum)
    mine = exchanged(new_momentum, (Z,)).reshape(-1, width)
    other = lax.ppermute(mine, CORE, [(0, 1), (1, 0)])
    here = mine.shape[0]
    (own,) = on_core(
        own_gram_kernel, [jax.ShapeDtypeStruct((here, here), jnp.float32)], [VMEM], [VMEM]
    )(mine)
    scale = 0.2 * width**0.5
    result, new_momentum = on_core(
        lambda *refs: orthogonal_kernel(scale, *refs),
        [jax.ShapeDtypeStruct(mine.shape, jnp.bfloat16), stack],
        [VMEM, VMEM, VMEM, VMEM],
        [VMEM, HBM],
        [
            pltpu.VMEM((2 * here, width), jnp.bfloat16),
            pltpu.VMEM((2 * here, 2 * here), jnp.float32),
            pltpu.SemaphoreType.DMA,
        ],
    )(mine, other, own, new_momentum)
    update = exchanged(result.reshape(grads.shape), (Z,))
    return (update, new_momentum)


def solution(mesh):
    torus = Mesh(mesh.devices.reshape(12, 2, 8, 4), ("fsdp_0", "fsdp_1", "grp_0", "grp_1"))
    in_specs = (P(GRP, FSDP, None), P(GRP, FSDP, None), P(GRP))
    out_specs = (P(GRP, FSDP, None), P(GRP, FSDP, None))
    return jax.shard_map(local, mesh=torus, in_specs=in_specs, out_specs=out_specs, check_vma=False)
```
